32 devices in a mesh: gx: 2 (over y), gy: 4 (over z), gz: 4 (over x, core).
Axes of the slice: x: 2, y: 2, z: 4, core: 2. Of those that a mesh axis runs over, the one named last changes fastest.
Arguments:
- forcing: float32 [3, 16, 64, 512], P(None, 'gx', 'gy', 'gz'), may hold values from -8 to 8
- viscosity: float32 [16, 64, 512], P('gx', 'gy', 'gz'), may hold values from 0.001 to 1000
Outputs:
- solution: float32 [3, 16, 64, 512], P(None, 'gx', 'gy', 'gz')
- residual: float32 [3, 16, 64, 512], P(None, 'gx', 'gy', 'gz')
The draws below stay inside these ranges and needn't reach their ends.
All inputs are finite; a program needn't handle non-finite values.
Results may differ from the reference program's by a relative error of at most 0.00017.
Values sent between devices are 32-bit elements; how exact they have to be, the bound alone decides.
A program may use at most 64 MiB of HBM per device.

```python
import math
import jax
import jax.numpy as jnp

ITERS = 3
CSWEEPS = 4
NX = 16
NY = 64
NZ = 512


def block_scale(stream_key, shape, split, smallest, high):
    gain = 1.0
    for dim, blocks in split:
        draws = jax.random.uniform(jax.random.fold_in(jax.random.fold_in(stream_key, 6), dim), (blocks,), jnp.float32, smallest / len(split), high / len(split))
        gain = gain * jnp.repeat(jnp.exp(draws), shape[dim] // blocks).reshape((-1,) + (1,) * (len(shape) - 1 - dim))
    return gain


def centred(stream_key, shape, width, reach, cuts=(), kind=jnp.bfloat16):
    gain = block_scale(stream_key, shape, cuts, -0.22, 0.18) if cuts else 1.0
    drawn = jax.random.normal(stream_key, shape, jnp.float32) * width * gain
    return jnp.minimum(jnp.maximum(drawn, -reach), reach).astype(kind)


def setup_inputs(seed: int = 0) -> dict:
    seeds = jax.random.split(jax.random.key(seed), 3)
    forcing = centred(seeds[0], (3, NX, NY, NZ), 1.0, 8.0, ((1, 2), (2, 4), (3, 4)), jnp.float32)
    viscosity = jnp.clip(jnp.exp(math.log(1000.0) - 13.815511 * jax.random.uniform(seeds[1], (NX, NY, NZ), jnp.float32) ** block_scale(seeds[1], (NX, NY, NZ), ((0, 2), (1, 4), (2, 4)), -0.2, 0.2)), 0.001, 1000.0)
    return dict(forcing=forcing, viscosity=viscosity)


reaction = 1.0
relaxation = 2.0 / 3.0
neighbours = ((1, 0, 0), (-1, 0, 0), (0, 1, 0), (0, -1, 0), (0, 0, 1), (0, 0, -1))


def window(padded, offset, extent):
    return padded[..., 1 + offset[0]:1 + offset[0] + extent[0], 1 + offset[1]:1 + offset[1] + extent[1], 1 + offset[2]:1 + offset[2] + extent[2]]


def viscous(values, padded_values, viscosity, padded_visc, mass_term, face_term):
    extent = viscosity.shape
    summed = mass_term * values
    for offset in neighbours:
        beside = window(padded_visc, offset, extent)
        across = window(padded_values, offset, extent)
        summed = summed + face_term * (viscosity + beside) * (values - across)
    return summed


def diagonal_of(viscosity, padded_visc, mass_term, face_term):
    summed = jnp.full(viscosity.shape, mass_term, jnp.float32)
    for offset in neighbours:
        summed = summed + face_term * (viscosity + window(padded_visc, offset, viscosity.shape))
    return summed


def restrict(values):
    extent = values.shape
    return values.reshape(extent[0], extent[1] // 2, 2, extent[2] // 2, 2, extent[3] // 2, 2).sum(axis=(2, 4, 6))


def prolong(values):
    return jnp.repeat(jnp.repeat(jnp.repeat(values, 2, axis=1), 2, axis=2), 2, axis=3)


def coarsen(viscosity):
    extent = viscosity.shape
    return viscosity.reshape(extent[0] // 2, 2, extent[1] // 2, 2, extent[2] // 2, 2).mean(axis=(1, 3, 5))


def sweeps(coarse_rhs, diagonal, applier):
    correction = relaxation * coarse_rhs / diagonal
    for counter in range(CSWEEPS - 1):
        correction = correction + relaxation * (coarse_rhs - applier(correction)) / diagonal
    return correction


def pad_all(values):
    return jnp.pad(values, ((0, 0), (1, 1), (1, 1), (1, 1)))


def reference(forcing, viscosity):
    padded_visc = jnp.pad(viscosity, 1)
    fine_diag = diagonal_of(viscosity, padded_visc, reaction, 0.5)
    coarse_visc = coarsen(viscosity)
    coarse_pad = jnp.pad(coarse_visc, 1)
    coarse_diag = diagonal_of(coarse_visc, coarse_pad, 8.0 * reaction, 2.0)

    def fine_apply(values):
        return viscous(values, pad_all(values), viscosity, padded_visc, reaction, 0.5)

    def coarse_apply(values):
        return viscous(values, pad_all(values), coarse_visc, coarse_pad, 8.0 * reaction, 2.0)

    def precondition(residual):
        smoothed = relaxation * residual / fine_diag
        defect = residual - fine_apply(smoothed)
        correction = sweeps(restrict(defect), coarse_diag, coarse_apply)
        smoothed = smoothed + prolong(correction)
        return smoothed + relaxation * (residual - fine_apply(smoothed)) / fine_diag

    solution = jnp.zeros_like(forcing)
    residual = forcing
    precond = precondition(residual)
    product = jnp.sum(residual * precond)
    direction = precond
    for iteration in range(ITERS):
        applied = fine_apply(direction)
        alpha_step = product / jnp.sum(direction * applied)
        solution = solution + alpha_step * direction
        residual = residual - alpha_step * applied
        if iteration + 1 < ITERS:
            precond = precondition(residual)
            product_next = jnp.sum(residual * precond)
            direction = precond + (product_next / product) * direction
            product = product_next
    return solution, residual
```

```python
import functools
import jax
import jax.numpy as jnp
from jax import lax
from jax.experimental import pallas as pl
from jax.experimental.pallas import tpu as pltpu
from jax.sharding import PartitionSpec as P

ITERS = 3
CSWEEPS = 4
AXES = ("gx", "gy", "gz")
MESH = pl.DeviceIdType.MESH
relax = 2.0 / 3.0
ROUNDS = 2 + ITERS * (CSWEEPS + 2)


def kernel(sizes, f_ref, v_ref, x_out, r_out, sx, sy, sz, rx, ry, rz, cf, fw, cc, cw, r, u, w, p, s, q, z,
           ssend, srecv, red_src, red_dst, rsend, rrecv):
    NC, X, Y, Z = f_ref.shape
    T = Y // 8
    place = [lax.axis_index(a) for a in AXES]
    total = [sizes[a] for a in AXES]
    gx_n, gy_n, gz_n = total
    plane = [(i, j) for i in range(gx_n) for j in range(gz_n) if (i, j) != (0, 0)]

    def plane_peer(i, j):
        return {"gx": lax.rem(place[0] + i, gx_n), "gz": lax.rem(place[2] + j, gz_n)}

    def line_peer(i):
        return {"gy": lax.rem(place[1] + i, gy_n)}

    barrier = pltpu.get_barrier_semaphore()
    count = len(plane) + gy_n - 1
    for i, j in plane:
        pl.semaphore_signal(barrier, inc=1, device_id=plane_peer(i, j), device_id_type=MESH)
    for i in range(1, gy_n):
        pl.semaphore_signal(barrier, inc=1, device_id=line_peer(i), device_id_type=MESH)

    for a, buf in enumerate((rx, ry, rz)):
        @pl.when(place[a] == 0)
        def _():
            buf[:, 0] = jnp.zeros_like(buf[:, 0])

        @pl.when(place[a] == total[a] - 1)
        def _():
            buf[:, 1] = jnp.zeros_like(buf[:, 1])

    lane2 = lax.broadcasted_iota(jnp.int32, (8, Z), 1)
    iy = lax.broadcasted_iota(jnp.int32, (1, Y, Z), 1)
    iz = lax.broadcasted_iota(jnp.int32, (1, Y, Z), 2)

    def copies(slot, nc):
        made = []
        for a, (src, dst) in enumerate(((sx, rx), (sy, ry), (sz, rz))):
            for up in (0, 1):
                ok = place[a] < total[a] - 1 if up else place[a] > 0
                if a == 2:
                    source, target = src.at[slot], dst.at[slot, 1 - up]
                else:
                    source = src.at[slot, up, pl.ds(0, nc)]
                    target = dst.at[slot, 1 - up, pl.ds(0, nc)]
                copy = pltpu.make_async_remote_copy(
                    src_ref=source, dst_ref=target, send_sem=ssend.at[slot, 2 * a + up],
                    recv_sem=srecv.at[slot, 2 * a + 1 - up],
                    device_id={AXES[a]: place[a] + (1 if up else -1)}, device_id_type=MESH)
                if a == 2:
                    mine = dst.at[slot, up]
                else:
                    mine = dst.at[slot, up, pl.ds(0, nc)]
                arrive = pltpu.make_async_remote_copy(
                    src_ref=source, dst_ref=mine, send_sem=ssend.at[slot, 2 * a + up],
                    recv_sem=srecv.at[slot, 2 * a + up],
                    device_id={AXES[a]: place[a] + (1 if up else -1)}, device_id_type=MESH)
                made.append((ok, copy, arrive))
        return made

    used = []

    def launch(slot, comps, unit):
        used.append((slot, len(comps)))
        nx = comps[0].shape[0]
        made = copies(slot, len(comps))
        for c, v in enumerate(comps):
            sx[slot, 0, c] = v[0]
            sx[slot, 1, c] = v[nx - 1]
        for ok, copy, _ in made[0:2]:
            pl.when(ok)(copy.start)
        for c, v in enumerate(comps):
            for i in range(X):
                k = i * nx // X
                sy[slot, 0, c, i : i + 1] = v[k, 0:1]
                sy[slot, 1, c, i : i + 1] = v[k, Y - 1 : Y]
        for ok, copy, _ in made[2:4]:
            pl.when(ok)(copy.start)
        which = (lane2 - unit + 2 * unit) // (2 * unit) - 1
        packed = jnp.zeros((8, Z), jnp.float32)
        for c, v in enumerate(comps):
            for i in range(nx):
                for t in range(T):
                    k = (c * nx + i) * T + t
                    rolled = pltpu.roll(v[i, 8 * t : 8 * t + 8], (2 * unit * (k + 1)) % Z, 1)
                    packed = jnp.where((lane2 >= 2 * unit * k + unit), rolled, packed)
        sz[slot] = packed
        for ok, copy, _ in made[4:6]:
            pl.when(ok)(copy.start)

    def land(slot, nc, nx, unit):
        for ok, _, arrive in copies(slot, nc):
            pl.when(ok)(arrive.wait_recv)
        below, above = rz[slot, 0], rz[slot, 1]
        both = jnp.where(lax.rem(lane2, 2 * unit) >= unit, below, pltpu.roll(above, Z - 2 * unit, 1))
        halos = []
        for c in range(nc):
            hz = []
            for i in range(nx):
                parts = []
                for t in range(T):
                    k = (c * nx + i) * T + t
                    parts.append(pltpu.roll(both, (2 * Z - unit - 2 * unit * k) % Z, 1))
                hz.append(jnp.concatenate(parts, axis=0)[None])
            hz = jnp.concatenate(hz, axis=0)
            halos.append((rx[slot, 0, c], rx[slot, 1, c], ry[slot, 0, c], ry[slot, 1, c], hz))
        return halos

    def rows(h, nx):
        h = h[:, None, :]
        if nx != X:
            h = jnp.concatenate([h[i * X // nx][None] for i in range(nx)], axis=0)
        return h

    def beside(v, halo, unit):
        nx = v.shape[0]
        hxm, hxp, hym, hyp, hz = halo
        return (
            jnp.concatenate([v[1:], hxp[None]], axis=0),
            jnp.concatenate([hxm[None], v[:-1]], axis=0),
            jnp.where(iy >= Y - unit, rows(hyp, nx), pltpu.roll(v, Y - unit, 1)),
            jnp.where(iy < unit, rows(hym, nx), pltpu.roll(v, unit, 1)),
            jnp.where(iz >= Z - unit, hz, pltpu.roll(v, Z - unit, 2)),
            jnp.where(iz < unit, hz, pltpu.roll(v, unit, 2)),
        )

    def viscous(v, halo, coef, mass, unit):
        out = v * mass if mass != 1.0 else v
        for d, across in enumerate(beside(v, halo, unit)):
            out = out + coef[d] * (v - across)
        return out

    def pairsum(v):
        v = v.reshape(X // 2, 2, Y, Z)
        v = v[:, 0] + v[:, 1]
        v = v + jnp.where(iy % 2 == 0, pltpu.roll(v, Y - 1, 1), pltpu.roll(v, 1, 1))
        return v + jnp.where(iz % 2 == 0, pltpu.roll(v, Z - 1, 2), pltpu.roll(v, 1, 2))

    def twice(v):
        h = v.shape[0]
        return jnp.broadcast_to(v[:, None], (h, 2) + v.shape[1:]).reshape((2 * h,) + v.shape[1:])

    C = range(NC)
    nxc = X // 2
    visc = v_ref[...]
    cvisc = pairsum(visc) * 0.125
    pl.semaphore_wait(barrier, count)
    launch(0, [visc], 1)
    launch(1, [cvisc], 2)

    (halo,) = land(0, 1, X, 1)
    diag = jnp.ones_like(visc)
    for d, other in enumerate(beside(visc, halo, 1)):
        face = 0.5 * (visc + other)
        cf[d] = face
        diag = diag + face
    fw[...] = relax / diag
    next_slot = [2]

    def take():
        next_slot[0] += 1
        return next_slot[0] - 1

    first = [True]

    def pair(vec, store_m, store_n, middle):
        a = take()
        sm = [vec[c] * fw[...] for c in C]
        launch(a, sm, 1)
        if first[0]:
            first[0] = False
            (ch,) = land(1, 1, nxc, 2)
            cdiag = jnp.full_like(cvisc, 8.0)
            for d, other in enumerate(beside(cvisc, ch, 2)):
                face = 2.0 * (cvisc + other)
                cc[d] = face
                cdiag = cdiag + face
            cw[...] = relax / cdiag
        fine_halo = land(a, NC, X, 1)
        rhs = [pairsum(vec[c] - viscous(sm[c], fine_halo[c], cf, 1.0, 1)) for c in C]
        corr = [rhs[c] * cw[...] for c in C]
        for sweep in range(CSWEEPS - 1):
            b = take()
            launch(b, corr, 2)
            if sweep == 1:
                middle()
            ch = land(b, NC, nxc, 2)
            corr = [corr[c] + cw[...] * (rhs[c] - viscous(corr[c], ch[c], cc, 8.0, 2)) for c in C]
        b = take()
        launch(b, corr, 2)
        ch = land(b, NC, nxc, 2)
        m = []
        for c in C:
            sm2 = sm[c] + twice(corr[c])
            halo = tuple(fine_halo[c][i] + ch[c][i] for i in range(4)) + (fine_halo[c][4] + twice(ch[c][4]),)
            m.append(sm2 + fw[...] * (vec[c] - viscous(sm2, halo, cf, 1.0, 1)))
        b = take()
        launch(b, m, 1)
        for c in C:
            store_m(c, m[c])
        mh = land(b, NC, X, 1)
        for c in C:
            store_n(c, viscous(m[c], mh[c], cf, 1.0, 1))

    def red_copy(n, stage, k):
        if stage == 0:
            i, j = plane[k]
            peer, base = plane_peer(i, j), k
        else:
            peer, base = line_peer(k + 1), len(plane) + k
        return pltpu.make_async_remote_copy(
            src_ref=red_src.at[n, stage], dst_ref=red_dst.at[n, base],
            send_sem=rsend.at[n, base], recv_sem=rrecv.at[n, base],
            device_id=peer, device_id_type=MESH)

    def peers(stage):
        return range(len(plane)) if stage == 0 else range(gy_n - 1)

    def fold(v):
        v = v.reshape(X * T, 8, Z).sum(axis=0)
        return v + pltpu.roll(v, 4, 0)

    sub = lax.broadcasted_iota(jnp.int32, (8, Z), 0)

    def reduce_start(n):
        g = d = 0.0
        for c in C:
            g = g + r[c] * u[c]
            d = d + u[c] * w[c]
        red_src[n, 0] = jnp.where(sub < 4, fold(g), fold(d))
        for k in peers(0):
            red_copy(n, 0, k).start()

    def reduce_middle(n):
        acc = red_src[n, 0]
        for k in peers(0):
            red_copy(n, 0, k).wait_recv()
            acc = acc + red_dst[n, k]
        red_src[n, 1] = acc
        for k in peers(1):
            red_copy(n, 1, k).start()

    def reduce_end(n):
        acc = red_src[n, 1]
        for k in peers(1):
            red_copy(n, 1, k).wait_recv()
            acc = acc + red_dst[n, len(plane) + k]
        g = jnp.sum(jnp.where(sub < 4, acc, 0.0))
        d = jnp.sum(jnp.where(sub < 4, 0.0, acc))
        return jnp.full((1, 1, Z), g), jnp.full((1, 1, Z), d)

    def put(ref):
        def store(c, value):
            ref[c] = value
        return store

    r[...] = f_ref[...]
    pair([f_ref[c] for c in C], put(u), put(w), lambda: None)
    gamma_old = alpha_old = None
    for n in range(ITERS):
        last = n == ITERS - 1
        reduce_start(n)
        fresh = {}
        if not last:
            store_m = lambda c, value: fresh.__setitem__(("m", c), value)
            store_n = lambda c, value: fresh.__setitem__(("n", c), value)
            pair([w[c] for c in C], store_m, store_n, lambda: reduce_middle(n))
        else:
            reduce_middle(n)
        gamma, delta = reduce_end(n)
        if n == 0:
            beta = None
            alpha = gamma / delta
        else:
            beta = gamma / gamma_old
            alpha = gamma / (delta - beta * gamma / alpha_old)
        mix = lambda new, ref, c: new if beta is None else new + beta * ref[c]
        for c in C:
            dn = mix(u[c], p, c)
            an = mix(w[c], s, c)
            x_out[c] = alpha * dn if n == 0 else x_out[c] + alpha * dn
            res = r[c] - alpha * an
            if last:
                r_out[c] = res
                continue
            r[c] = res
            p[c] = dn
            s[c] = an
            qn = mix(fresh["m", c], q, c)
            zn = mix(fresh["n", c], z, c)
            q[c] = qn
            z[c] = zn
            u[c] = u[c] - alpha * qn
            w[c] = w[c] - alpha * zn
        gamma_old, alpha_old = gamma, alpha

    for slot, nc in used:
        for ok, copy, _ in copies(slot, nc):
            pl.when(ok)(copy.wait_send)
    for n in range(ITERS):
        for stage in (0, 1):
            for k in peers(stage):
                red_copy(n, stage, k).wait_send()


def solution(mesh):
    sizes = dict(mesh.shape)

    def shards(forcing, viscosity):
        NC, X, Y, Z = forcing.shape
        f32 = jnp.float32
        whole = pltpu.VMEM((NC, X, Y, Z), f32)
        peers = sizes["gx"] * sizes["gz"] - 1 + sizes["gy"] - 1
        spec = pl.BlockSpec(memory_space=pltpu.VMEM)
        out = jax.ShapeDtypeStruct(forcing.shape, f32)
        dma = pltpu.SemaphoreType.DMA
        halo = [
            pltpu.VMEM((ROUNDS, 2, NC, Y, Z), f32),
            pltpu.VMEM((ROUNDS, 2, NC, X, Z), f32),
        ]
        return pl.pallas_call(
            functools.partial(kernel, sizes),
            out_shape=(out, out),
            in_specs=[spec, spec],
            out_specs=(spec, spec),
            scratch_shapes=halo + [pltpu.VMEM((ROUNDS, 8, Z), f32)] + halo + [
                pltpu.VMEM((ROUNDS, 2, 8, Z), f32),
                pltpu.VMEM((6, X, Y, Z), f32),
                pltpu.VMEM((X, Y, Z), f32),
                pltpu.VMEM((6, X // 2, Y, Z), f32),
                pltpu.VMEM((X // 2, Y, Z), f32),
            ] + [whole] * 7 + [
                dma((ROUNDS, 6)),
                dma((ROUNDS, 6)),
                pltpu.VMEM((ITERS, 2, 8, Z), f32),
                pltpu.VMEM((ITERS, peers, 8, Z), f32),
                dma((ITERS, peers)),
                dma((ITERS, peers)),
            ],
            compiler_params=pltpu.CompilerParams(
                collective_id=0, has_side_effects=True, vmem_limit_bytes=48 * 1024 * 1024
            ),
        )(forcing, viscosity)

    return jax.shard_map(
        shards,
        mesh=mesh,
        in_specs=(P(None, "gx", "gy", "gz"), P("gx", "gy", "gz")),
        out_specs=(P(None, "gx", "gy", "gz"), P(None, "gx", "gy", "gz")),
        check_vma=False,
    )
```

```python
import functools
import jax
import jax.numpy as jnp
from jax import lax
from jax.experimental import pallas as pl
from jax.experimental.pallas import tpu as pltpu
from jax.sharding import PartitionSpec as P

ITERS = 3
AXES = ("gx", "gy", "gz")
MESH = pl.DeviceIdType.MESH
relax = 2.0 / 3.0
ROUNDS = 3 + 3 * ITERS
BESIDE = [(0, 0), (0, 1), (1, 0), (1, 1)]


def kernel(sizes, f_ref, v_ref, x_out, r_out, sx, sy, sz, sxy, syz, rx, ry, rz, rxy, ryz, rxz,
           cfE, cfY, cfZ, fwE, fwY, fwZ, ccE, ccY, ccZ, cwE, cwY, cwZ,
           ssend, srecv, red_src, red_dst, rsend, rrecv):
    NC, X, Y, Z = f_ref.shape
    T = Y // 8
    C = range(NC)
    place = [lax.axis_index(a) for a in AXES]
    total = [sizes[a] for a in AXES]
    gx_n, gy_n, gz_n = total
    plane = [(i, j) for i in range(gx_n) for j in range(gz_n) if (i, j) != (0, 0)]

    def plane_peer(i, j):
        return {"gx": lax.rem(place[0] + i, gx_n), "gz": lax.rem(place[2] + j, gz_n)}

    def line_peer(i):
        return {"gy": lax.rem(place[1] + i, gy_n)}

    def exists(offset):
        ok = None
        for a in range(3):
            if offset[a]:
                here = place[a] < total[a] - 1 if offset[a] > 0 else place[a] > 0
                ok = here if ok is None else jnp.logical_and(ok, here)
        return ok

    def peer_at(offset):
        return {AXES[a]: place[a] + offset[a] for a in range(3) if offset[a]}

    def side(up):
        return 1 if up else -1

    faces = [tuple(side(up) if a == b else 0 for b in range(3)) for a in range(3) for up in (0, 1)]
    pairs = ((0, 1), (1, 2), (0, 2))
    edges = [(pair_, i, j) for pair_ in pairs for i, j in BESIDE]

    def edge_offset(edge):
        (a, b), i, j = edge
        return tuple(side(i) if d == a else side(j) if d == b else 0 for d in range(3))

    barrier = pltpu.get_barrier_semaphore()
    for i, j in plane:
        pl.semaphore_signal(barrier, inc=1, device_id=plane_peer(i, j), device_id_type=MESH)
    for i in range(1, gy_n):
        pl.semaphore_signal(barrier, inc=1, device_id=line_peer(i), device_id_type=MESH)
    count = len(plane) + gy_n - 1
    for edge in edges:
        if edge[0] != (0, 2):
            ok, to = exists(edge_offset(edge)), peer_at(edge_offset(edge))

            @pl.when(ok)
            def _():
                pl.semaphore_signal(barrier, inc=1, device_id=to, device_id_type=MESH)

            count = count + ok.astype(jnp.int32)

    for a, buf in enumerate((rx, ry, rz)):
        for up in (0, 1):
            @pl.when(jnp.logical_not(exists(faces[2 * a + up])))
            def _():
                buf[:, up] = jnp.zeros_like(buf[:, up])
    for n, buf in enumerate((rxy, ryz, rxz)):
        for e in range(4):
            @pl.when(jnp.logical_not(exists(edge_offset(edges[4 * n + e]))))
            def _():
                buf[:, e] = jnp.zeros_like(buf[:, e])

    lane = lax.broadcasted_iota(jnp.int32, (8, Z), 1)
    sub = lax.broadcasted_iota(jnp.int32, (8, Z), 0)
    iy = lax.broadcasted_iota(jnp.int32, (1, Y, Z), 1)
    iz = lax.broadcasted_iota(jnp.int32, (1, Y, Z), 2)

    def copies(slot, nc, nx):
        fine = nx == X
        planes = 2 * nc if fine else 2
        rows_n = 2 * nc
        made = []

        def make(n, offset, src, dst, mine, opposite):
            made.append((n, exists(offset),
                pltpu.make_async_remote_copy(
                    src_ref=src, dst_ref=dst, send_sem=ssend.at[slot, n],
                    recv_sem=srecv.at[slot, opposite], device_id=peer_at(offset), device_id_type=MESH),
                pltpu.make_async_remote_copy(
                    src_ref=src, dst_ref=mine, send_sem=ssend.at[slot, n],
                    recv_sem=srecv.at[slot, n], device_id=peer_at(offset), device_id_type=MESH)))

        for n, offset in enumerate(faces):
            a, up = n // 2, n % 2
            if a == 0:
                cut = pl.ds(0, planes)
                make(n, offset, sx.at[slot, up, cut], rx.at[slot, 1 - up, cut], rx.at[slot, up, cut], n ^ 1)
            elif a == 1:
                cut = pl.ds(0, rows_n)
                make(n, offset, sy.at[slot, up, cut], ry.at[slot, 1 - up, cut], ry.at[slot, up, cut], n ^ 1)
            else:
                make(n, offset, sz.at[slot], rz.at[slot, 1 - up], rz.at[slot, up], n ^ 1)
        for m, edge in enumerate(edges):
            pair_, i, j = edge
            e, far = 2 * i + j, 2 * (1 - i) + (1 - j)
            n, opposite = 6 + m, 6 + 4 * (m // 4) + far
            if pair_ == (0, 1):
                src, dst = sxy.at[slot, e], rxy
            elif pair_ == (1, 2):
                src, dst = syz.at[slot, i], ryz
            else:
                src, dst = sz.at[slot], rxz
            make(n, edge_offset(edge), src, dst.at[slot, far], dst.at[slot, e], opposite)
        return made

    used = []

    def go(made, which):
        for n, ok, copy, _ in made:
            if n in which:
                pl.when(ok)(copy.start)

    def launch(slot, comps, unit):
        nc, nx = len(comps), comps[0].shape[0]
        used.append((slot, nc, nx))
        made = copies(slot, nc, nx)
        for up in (0, 1):
            for layer in (0, 1):
                k = nx - 1 - layer if up else layer
                if nx == X:
                    for c in range(nc):
                        sx[slot, up, layer * nc + c] = comps[c][k]
                else:
                    flat = comps[0][k]
                    if nc > 1:
                        flat = jnp.where(iy[0] % 2 == 1, comps[1][k], flat)
                    if nc > 2:
                        flat = jnp.where(iz[0] % 2 == 1, comps[2][k], flat)
                    sx[slot, up, layer] = flat
        go(made, (0, 1))
        for up in (0, 1):
            for c, v in enumerate(comps):
                for i in range(X):
                    k = i * nx // X
                    for layer in (0, 1):
                        row = Y - 1 - layer * unit if up else layer * unit
                        sy[slot, up, layer * nc + c, i : i + 1] = v[k, row : row + 1]
                    if i in (0, X - 1):
                        sxy[slot, (2 if i else 0) + up, c : c + 1] = v[k, Y - 1 if up else 0][None]
        go(made, (2, 3, 6, 7, 8, 9))
        wide = 4 * unit
        for t in range(T):
            packed = jnp.zeros((8, Z), jnp.float32)
            for c, v in enumerate(comps):
                for i in range(nx):
                    at = wide * (c * nx + i)
                    rolled = pltpu.roll(v[i, 8 * t : 8 * t + 8], (at + 2 * unit) % Z, 1)
                    packed = jnp.where(lane >= at, rolled, packed)
            sz[slot, t] = packed
        go(made, (4, 5, 14, 15, 16, 17))
        for up in (0, 1):
            packed = jnp.zeros((8, Z), jnp.float32)
            for c in range(nc):
                at = wide * c * nx
                rolled = pltpu.roll(sy[slot, up, c], (at + 2 * unit) % Z, 1)
                packed = jnp.where(lane >= at, rolled, packed)
            syz[slot, up] = packed
        go(made, (10, 11, 12, 13))

    def rot(v, amount, axis):
        amount = amount % v.shape[axis]
        return pltpu.roll(v, amount, axis) if amount else v

    def near(below, above, unit):
        return jnp.where(lane % (4 * unit) < unit, rot(above, -2 * unit, 1), below)

    def unpack(tile, k, unit):
        return rot(tile, -unit - 4 * unit * k, 1)

    def stack(parts):
        return jnp.concatenate([q_[None] for q_ in parts], axis=0)

    def column(tiles, k, unit):
        return jnp.concatenate([unpack(tile, k, unit) for tile in tiles], axis=0)

    def six(v, hxm, hxp, hym, hyp, hz, unit):
        return (
            jnp.concatenate([v[1:], hxp[None]], axis=0),
            jnp.concatenate([hxm[None], v[:-1]], axis=0),
            jnp.where(iy >= Y - unit, hyp, pltpu.roll(v, Y - unit, 1)),
            jnp.where(iy < unit, hym, pltpu.roll(v, unit, 1)),
            jnp.where(iz >= Z - unit, hz, pltpu.roll(v, Z - unit, 2)),
            jnp.where(iz < unit, hz, pltpu.roll(v, unit, 2)),
        )

    def slab_rows(slab, nx):
        return [slab[i * X // nx : i * X // nx + 1] for i in range(nx)]

    def expand(flat, c):
        odd_z = iz[0] % 2 == 1
        odd_y = iy[0] % 2 == 1
        v = jnp.where(odd_z, flat, rot(flat, -1, 1)) if c == 2 else jnp.where(odd_z, rot(flat, 1, 1), flat)
        return jnp.where(odd_y, v, rot(v, -1, 0)) if c == 1 else jnp.where(odd_y, rot(v, 1, 0), v)

    def land(slot, comps, unit):
        nc, nx = len(comps), comps[0].shape[0]
        for n, ok, _, arrive in copies(slot, nc, nx):
            pl.when(ok)(arrive.wait_recv)
        wide = 4 * unit

        def xplane(c, up, layer):
            if nx == X:
                return rx[slot, up, layer * nc + c]
            flat = rx[slot, up, layer]
            if nc == 1:
                return flat
            return expand(flat, c)

        H1 = [near(rz[slot, 0, t], rz[slot, 1, t], unit) for t in range(T)]
        H2 = [jnp.where(lane % wide < unit, rot(rz[slot, 1, t], -3 * unit, 1), rot(rz[slot, 0, t], unit, 1))
              for t in range(T)]
        EX = [[near(rxz[slot, 2 * a, t], rxz[slot, 2 * a + 1, t], unit) for t in range(T)] for a in (0, 1)]
        EY = [near(ryz[slot, 2 * b], ryz[slot, 2 * b + 1], unit) for b in (0, 1)]
        field = {"E": [], "Y": [], "Z": H1}
        nbs = {"E": [], "Y": [], "Z": []}
        ux = X // nx
        for c, v in enumerate(comps):
            ext = jnp.concatenate([xplane(c, 0, 0)[None], v, xplane(c, 1, 0)[None]], axis=0)
            hy = []
            for b in (0, 1):
                hy.append(stack([rxy[slot, b, c : c + 1]] + slab_rows(ry[slot, b, c], nx) + [rxy[slot, 2 + b, c : c + 1]]))
            hz = stack([column(EX[0], c * nx + nx - 1, unit)] + [column(H1, c * nx + i, unit) for i in range(nx)]
                       + [column(EX[1], c * nx, unit)])
            field["E"].append(ext)
            nbs["E"].append(six(ext, xplane(c, 0, 1), xplane(c, 1, 1), hy[0], hy[1], hz, unit))
            fy, ny = [], []
            for b in (0, 1):
                slab = ry[slot, b, c]
                out, inner = ry[slot, b, nc + c], sy[slot, b, c]
                hzs = unpack(EY[b], c * nx, unit)
                fy.append(slab)
                ny.append((
                    jnp.where(sub >= 8 - ux, rxy[slot, 2 + b, c : c + 1], rot(slab, -ux, 0)),
                    jnp.where(sub < ux, rxy[slot, b, c : c + 1], rot(slab, ux, 0)),
                    out, inner,
                    jnp.where(lane >= Z - unit, hzs, rot(slab, -unit, 1)),
                    jnp.where(lane < unit, hzs, rot(slab, unit, 1)),
                ))
            field["Y"].append(fy)
            nbs["Y"].append(ny)
        which = lane // wide % nx
        rim = []
        for b in (0, 1):
            line = jnp.zeros((1, Z), jnp.float32)
            for i in range(nx):
                row = EY[b][i * ux : i * ux + 1]
                line = jnp.where(which[0:1] == i, rot(row, wide * i, 1), line)
            rim.append(line)
        for t in range(T):
            h = H1[t]
            before = rim[0] if t == 0 else rot(H1[t - 1], unit, 0)
            after = rim[1] if t == T - 1 else rot(H1[t + 1], -unit, 0)
            nbs["Z"].append((
                jnp.where(which == nx - 1, rot(EX[1][t], wide * (nx - 1), 1), rot(h, -wide, 1)),
                jnp.where(which == 0, rot(EX[0][t], -wide * (nx - 1), 1), rot(h, wide, 1)),
                jnp.where(sub >= 8 - unit, after, rot(h, -unit, 0)),
                jnp.where(sub < unit, before, rot(h, unit, 0)),
                H2[t],
                rot(sz[slot, t], -unit, 1),
            ))
        return field, nbs

    def stencil(v, nb, coef, mass):
        out = v * mass if mass != 1.0 else v
        for d in range(6):
            out = out + coef[d] * (v - nb[d])
        return out

    def viscous_wide(field, nbs, coefs, mass):
        cE, cY, cZ = coefs
        return {
            "E": [stencil(v, nb, cE, mass) for v, nb in zip(field["E"], nbs["E"])],
            "Y": [[stencil(f[b], n[b], cY[b], mass) for b in (0, 1)] for f, n in zip(field["Y"], nbs["Y"])],
            "Z": [stencil(field["Z"][t], nbs["Z"][t], [cZ[d, t] for d in range(6)], mass) for t in range(T)],
        }

    def viscous(field, coefs, mass, unit):
        out = []
        for c in C:
            ext = field["E"][c]
            nx = ext.shape[0] - 2
            hy = [stack(slab_rows(field["Y"][c][b], nx)) for b in (0, 1)]
            hz = stack([column(field["Z"], c * nx + i, unit) for i in range(nx)])
            v = ext[1 : nx + 1]
            nb = six(v, ext[0], ext[nx + 1], hy[0], hy[1], hz, unit)
            out.append(stencil(v, nb, [coefs[0][d, 1 : nx + 1] for d in range(6)], mass))
        return out

    def fmap(fn, *fields):
        return {
            "E": [fn(*parts) for parts in zip(*(f["E"] for f in fields))],
            "Y": [[fn(*(f["Y"][c][b] for f in fields)) for b in (0, 1)] for c in range(len(fields[0]["Y"]))],
            "Z": [fn(*parts) for parts in zip(*(f["Z"] for f in fields))],
        }

    def flat_row(scalar, like):
        return scalar if like.ndim == 3 else scalar[0]

    def weights(E, Yw, Zw):
        return {"E": [E[...]] * NC, "Y": [[Yw[b] for b in (0, 1)]] * NC, "Z": [Zw[t] for t in range(T)]}

    def core(field):
        return [e[1 : e.shape[0] - 1] for e in field["E"]]

    def pairsum(v):
        v = v.reshape(X // 2, 2, Y, Z)
        v = v[:, 0] + v[:, 1]
        v = v + jnp.where(iy % 2 == 0, pltpu.roll(v, Y - 1, 1), pltpu.roll(v, 1, 1))
        return v + jnp.where(iz % 2 == 0, pltpu.roll(v, Z - 1, 2), pltpu.roll(v, 1, 2))

    def prolong(field):
        def deep(e):
            n = e.shape[0] - 2
            return jnp.concatenate([e[0:1]] + [e[1 + i : 2 + i] for i in range(n) for _ in (0, 1)] + [e[n + 1 :]], axis=0)

        def thin(h):
            m = lane % 8
            return jnp.where(m == 0, h, jnp.where(m == 1, rot(h, -1, 1), jnp.where(m == 4, rot(h, 4, 1), rot(h, 3, 1))))

        return {"E": [deep(e) for e in field["E"]], "Y": field["Y"], "Z": [thin(h) for h in field["Z"]]}

    inside = [jnp.where(exists(f), 1.0, 0.0).astype(jnp.float32) for f in faces]

    def set_up(field, nbs, nx, unit, mass, scale, E, Yc, Zc, wE, wY, wZ):
        v = field["E"][0]
        ix = lax.broadcasted_iota(jnp.int32, v.shape, 0)
        keep = jnp.where(ix == 0, inside[0], jnp.where(ix == nx + 1, inside[1], 1.0))
        diag = jnp.full(v.shape, mass, jnp.float32)
        for d in range(6):
            face = scale * (v + nbs["E"][0][d]) * keep
            E[d] = face
            diag = diag + face
        wE[...] = relax / diag
        for b in (0, 1):
            v = field["Y"][0][b]
            diag = jnp.full(v.shape, mass, jnp.float32)
            for d in range(6):
                face = scale * (v + nbs["Y"][0][b][d]) * inside[2 + b]
                Yc[b, d] = face
                diag = diag + face
            wY[b] = relax / diag
        keep = jnp.where(lane % (4 * unit) < unit, inside[5], inside[4])
        span = 4 * unit * nx
        for t in range(T):
            v = field["Z"][t]
            diag = jnp.full(v.shape, mass, jnp.float32)
            for d in range(6):
                face = scale * (v + nbs["Z"][t][d]) * keep
                each = face
                for c in range(1, NC):
                    each = jnp.where(lane >= c * span, rot(face, c * span, 1), each)
                Zc[d, t] = each
                diag = diag + each
            wZ[t] = relax / diag

    fine = (cfE, cfY, cfZ)
    coarse = (ccE, ccY, ccZ)
    visc = v_ref[...]
    cvisc = pairsum(visc) * 0.125
    force = [f_ref[c] for c in C]
    pl.semaphore_wait(barrier, count)
    launch(0, [visc], 1)
    launch(1, force, 1)
    launch(2, [cvisc], 2)
    field, nbs = land(0, [visc], 1)
    set_up(field, nbs, X, 1, 1.0, 0.5, cfE, cfY, cfZ, fwE, fwY, fwZ)
    field, nbs = land(2, [cvisc], 2)
    set_up(field, nbs, X // 2, 2, 8.0, 2.0, ccE, ccY, ccZ, cwE, cwY, cwZ)
    forced, _ = land(1, force, 1)
    next_slot = [3]

    def take():
        next_slot[0] += 1
        return next_slot[0] - 1

    def pair(vec, middle):
        fw = weights(fwE, fwY, fwZ)
        cw = weights(cwE, cwY, cwZ)
        nxc = X // 2
        sm = fmap(lambda a, b: a * b, vec, fw)
        applied = viscous(sm, fine, 1.0, 1)
        cwl = cwE[1 : nxc + 1]
        local = core(vec)
        first = [cwl * pairsum(local[c] - applied[c]) for c in C]
        slot = take()
        launch(slot, first, 2)
        one, nbs = land(slot, first, 2)
        two = fmap(lambda a, b, k: a + a - k * b, one, viscous_wide(one, nbs, coarse, 8.0), cw)
        applied = viscous(two, coarse, 8.0, 2)
        three = [v + first[c] - cwl * applied[c] for c, v in enumerate(core(two))]
        slot = take()
        launch(slot, three, 2)
        middle()
        field, nbs = land(slot, three, 2)
        four = fmap(lambda a, o, b, k: a + o - k * b, field, one, viscous_wide(field, nbs, coarse, 8.0), cw)
        sm = fmap(lambda a, b: a + b, sm, prolong(four))
        applied = viscous(sm, fine, 1.0, 1)
        fwl = fwE[1 : X + 1]
        m = [v + fwl * (local[c] - applied[c]) for c, v in enumerate(core(sm))]
        slot = take()
        launch(slot, m, 1)
        field, nbs = land(slot, m, 1)
        return m, viscous_wide(field, nbs, fine, 1.0)

    def red_copy(n, stage, k):
        if stage == 0:
            i, j = plane[k]
            peer, base = plane_peer(i, j), k
        else:
            peer, base = line_peer(k + 1), len(plane) + k
        return pltpu.make_async_remote_copy(
            src_ref=red_src.at[n, stage], dst_ref=red_dst.at[n, base],
            send_sem=rsend.at[n, base], recv_sem=rrecv.at[n, base],
            device_id=peer, device_id_type=MESH)

    def peers(stage):
        return range(len(plane)) if stage == 0 else range(gy_n - 1)

    def fold(v):
        v = v.reshape(X * T, 8, Z).sum(axis=0)
        return v + pltpu.roll(v, 4, 0)

    def reduce_start(n, r, u, w):
        g = d = 0.0
        for c in C:
            g = g + r[c] * u[c]
            d = d + u[c] * w[c]
        red_src[n, 0] = jnp.where(sub < 4, fold(g), fold(d))
        for k in peers(0):
            red_copy(n, 0, k).start()

    def reduce_middle(n):
        acc = red_src[n, 0]
        for k in peers(0):
            red_copy(n, 0, k).wait_recv()
            acc = acc + red_dst[n, k]
        red_src[n, 1] = acc
        for k in peers(1):
            red_copy(n, 1, k).start()

    def reduce_end(n):
        acc = red_src[n, 1]
        for k in peers(1):
            red_copy(n, 1, k).wait_recv()
            acc = acc + red_dst[n, len(plane) + k]
        g = jnp.sum(jnp.where(sub < 4, acc, 0.0))
        d = jnp.sum(jnp.where(sub < 4, 0.0, acc))
        return jnp.full((1, 1, Z), g), jnp.full((1, 1, Z), d)

    u, w = pair(forced, lambda: None)
    r = force
    gamma_old = alpha_old = None
    for n in range(ITERS):
        last = n == ITERS - 1
        wl = core(w)
        reduce_start(n, r, u, wl)
        if last:
            reduce_middle(n)
        else:
            m, nn = pair(w, lambda: reduce_middle(n))
        gamma, delta = reduce_end(n)
        if n == 0:
            alpha = gamma / delta
            p, s = u, wl
        else:
            beta = gamma / gamma_old
            alpha = gamma / (delta - beta * gamma / alpha_old)
            p = [u[c] + beta * p[c] for c in C]
            s = [wl[c] + beta * s[c] for c in C]
        for c in C:
            x_out[c] = alpha * p[c] if n == 0 else x_out[c] + alpha * p[c]
        r = [r[c] - alpha * s[c] for c in C]
        if last:
            for c in C:
                r_out[c] = r[c]
            break
        if n == 0:
            q, z = m, nn
        else:
            q = [m[c] + beta * q[c] for c in C]
            z = fmap(lambda a, b: a + flat_row(beta, a) * b, nn, z)
        u = [u[c] - alpha * q[c] for c in C]
        w = fmap(lambda a, b: a - flat_row(alpha, a) * b, w, z)
        gamma_old, alpha_old = gamma, alpha

    for slot, nc, nx in used:
        for _, ok, copy, _ in copies(slot, nc, nx):
            pl.when(ok)(copy.wait_send)
    for n in range(ITERS):
        for stage in (0, 1):
            for k in peers(stage):
                red_copy(n, stage, k).wait_send()


def solution(mesh):
    sizes = dict(mesh.shape)

    def shards(forcing, viscosity):
        NC, X, Y, Z = forcing.shape
        T = Y // 8
        f32 = jnp.float32
        peers = sizes["gx"] * sizes["gz"] - 1 + sizes["gy"] - 1
        spec = pl.BlockSpec(memory_space=pltpu.VMEM)
        out = jax.ShapeDtypeStruct(forcing.shape, f32)
        dma = pltpu.SemaphoreType.DMA
        V = lambda *shape: pltpu.VMEM(shape, f32)
        coefs = lambda nx: [V(6, nx + 2, Y, Z), V(2, 6, 8, Z), V(6, T, 8, Z)]
        weights = lambda nx: [V(nx + 2, Y, Z), V(2, 8, Z), V(T, 8, Z)]
        halo = [V(ROUNDS, 2, 2 * NC, Y, Z), V(ROUNDS, 2, 2 * NC, 8, Z)]
        return pl.pallas_call(
            functools.partial(kernel, sizes),
            out_shape=(out, out),
            in_specs=[spec, spec],
            out_specs=(spec, spec),
            scratch_shapes=halo + [V(ROUNDS, T, 8, Z), V(ROUNDS, 4, 8, Z), V(ROUNDS, 2, 8, Z)]
            + halo + [V(ROUNDS, 2, T, 8, Z), V(ROUNDS, 4, 8, Z), V(ROUNDS, 4, 8, Z), V(ROUNDS, 4, T, 8, Z)]
            + coefs(X) + weights(X) + coefs(X // 2) + weights(X // 2) + [
                dma((ROUNDS, 18)),
                dma((ROUNDS, 18)),
                V(ITERS, 2, 8, Z),
                V(ITERS, peers, 8, Z),
                dma((ITERS, peers)),
                dma((ITERS, peers)),
            ],
            compiler_params=pltpu.CompilerParams(
                collective_id=0, has_side_effects=True, vmem_limit_bytes=48 * 1024 * 1024
            ),
        )(forcing, viscosity)

    return jax.shard_map(
        shards,
        mesh=mesh,
        in_specs=(P(None, "gx", "gy", "gz"), P("gx", "gy", "gz")),
        out_specs=(P(None, "gx", "gy", "gz"), P(None, "gx", "gy", "gz")),
        check_vma=False,
    )
```

```python
import functools
import jax
import jax.numpy as jnp
from jax import lax
from jax.experimental import pallas as pl
from jax.experimental.pallas import tpu as pltpu
from jax.sharding import PartitionSpec as P

ITERS = 3
AXES = ("gx", "gy", "gz")
MESH = pl.DeviceIdType.MESH
relax = 2.0 / 3.0
ROUNDS = 3 + 3 * ITERS
BESIDE = [(0, 0), (0, 1), (1, 0), (1, 1)]


def kernel(sizes, f_ref, v_ref, x_out, r_out, sx, sy, sz, sxy, syz, rx, ry, rz, rxy, ryz, rxz,
           cfE, cfY, cfZ, fwE, fwY, fwZ, ccE, ccY, ccZ, cwE, cwY, cwZ, fin, frim, cin, crim,
           ssend, srecv, red_src, red_dst, rsend, rrecv):
    NC, X, Y, Z = f_ref.shape
    T = Y // 8
    C = range(NC)
    place = [lax.axis_index(a) for a in AXES]
    total = [sizes[a] for a in AXES]
    gx_n, gy_n, gz_n = total
    plane = [(i, j) for i in range(gx_n) for j in range(gz_n) if (i, j) != (0, 0)]

    def plane_peer(i, j):
        return {"gx": lax.rem(place[0] + i, gx_n), "gz": lax.rem(place[2] + j, gz_n)}

    def line_peer(i):
        return {"gy": lax.rem(place[1] + i, gy_n)}

    def exists(offset):
        ok = None
        for a in range(3):
            if offset[a]:
                here = place[a] < total[a] - 1 if offset[a] > 0 else place[a] > 0
                ok = here if ok is None else jnp.logical_and(ok, here)
        return ok

    def peer_at(offset):
        return {AXES[a]: place[a] + offset[a] for a in range(3) if offset[a]}

    def side(up):
        return 1 if up else -1

    faces = [tuple(side(up) if a == b else 0 for b in range(3)) for a in range(3) for up in (0, 1)]
    pairs = ((0, 1), (1, 2), (0, 2))
    edges = [(pair_, i, j) for pair_ in pairs for i, j in BESIDE]

    def edge_offset(edge):
        (a, b), i, j = edge
        return tuple(side(i) if d == a else side(j) if d == b else 0 for d in range(3))

    barrier = pltpu.get_barrier_semaphore()
    for i, j in plane:
        pl.semaphore_signal(barrier, inc=1, device_id=plane_peer(i, j), device_id_type=MESH)
    for i in range(1, gy_n):
        pl.semaphore_signal(barrier, inc=1, device_id=line_peer(i), device_id_type=MESH)
    count = len(plane) + gy_n - 1
    for edge in edges:
        if edge[0] != (0, 2):
            ok, to = exists(edge_offset(edge)), peer_at(edge_offset(edge))

            @pl.when(ok)
            def _():
                pl.semaphore_signal(barrier, inc=1, device_id=to, device_id_type=MESH)

            count = count + ok.astype(jnp.int32)

    for a, buf in enumerate((rx, ry, rz)):
        for up in (0, 1):
            @pl.when(jnp.logical_not(exists(faces[2 * a + up])))
            def _():
                buf[:, up] = jnp.zeros_like(buf[:, up])
    for n, buf in enumerate((rxy, ryz, rxz)):
        for e in range(4):
            @pl.when(jnp.logical_not(exists(edge_offset(edges[4 * n + e]))))
            def _():
                buf[:, e] = jnp.zeros_like(buf[:, e])

    lane = lax.broadcasted_iota(jnp.int32, (8, Z), 1)
    sub = lax.broadcasted_iota(jnp.int32, (8, Z), 0)
    iy = lax.broadcasted_iota(jnp.int32, (1, Y, Z), 1)
    iz = lax.broadcasted_iota(jnp.int32, (1, Y, Z), 2)

    def copies(slot, nc, nx):
        fine = nx == X
        planes = 2 * nc if fine else 2
        rows_n = 2 * nc
        made = []

        def make(n, offset, src, dst, mine, opposite):
            made.append((n, exists(offset),
                pltpu.make_async_remote_copy(
                    src_ref=src, dst_ref=dst, send_sem=ssend.at[slot, n],
                    recv_sem=srecv.at[slot, opposite], device_id=peer_at(offset), device_id_type=MESH),
                pltpu.make_async_remote_copy(
                    src_ref=src, dst_ref=mine, send_sem=ssend.at[slot, n],
                    recv_sem=srecv.at[slot, n], device_id=peer_at(offset), device_id_type=MESH)))

        for n, offset in enumerate(faces):
            a, up = n // 2, n % 2
            if a == 0:
                cut = pl.ds(0, planes)
                make(n, offset, sx.at[slot, up, cut], rx.at[slot, 1 - up, cut], rx.at[slot, up, cut], n ^ 1)
            elif a == 1:
                cut = pl.ds(0, rows_n)
                make(n, offset, sy.at[slot, up, cut], ry.at[slot, 1 - up, cut], ry.at[slot, up, cut], n ^ 1)
            else:
                make(n, offset, sz.at[slot], rz.at[slot, 1 - up], rz.at[slot, up], n ^ 1)
        for m, edge in enumerate(edges):
            pair_, i, j = edge
            e, far = 2 * i + j, 2 * (1 - i) + (1 - j)
            n, opposite = 6 + m, 6 + 4 * (m // 4) + far
            if pair_ == (0, 1):
                src, dst = sxy.at[slot, e], rxy
            elif pair_ == (1, 2):
                src, dst = syz.at[slot, i], ryz
            else:
                src, dst = sz.at[slot], rxz
            make(n, edge_offset(edge), src, dst.at[slot, far], dst.at[slot, e], opposite)
        return made

    used = []

    def go(made, which):
        for n in which:
            pl.when(made[n][1])(made[n][2].start)

    def launch(slot, comps, unit):
        nc, nx = len(comps), comps[0].shape[0]
        used.append((slot, nc, nx))
        made = copies(slot, nc, nx)
        for up in (0, 1):
            for layer in (0, 1):
                k = nx - 1 - layer if up else layer
                if nx == X:
                    for c in range(nc):
                        sx[slot, up, layer * nc + c] = comps[c][k]
                else:
                    flat = comps[0][k]
                    if nc > 1:
                        flat = jnp.where(iy[0] % 2 == 1, comps[1][k], flat)
                    if nc > 2:
                        flat = jnp.where(iz[0] % 2 == 1, comps[2][k], flat)
                    sx[slot, up, layer] = flat
        for up in (0, 1):
            for c, v in enumerate(comps):
                for i in range(X):
                    k = i * nx // X
                    for layer in (0, 1):
                        row = Y - 1 - layer * unit if up else layer * unit
                        sy[slot, up, layer * nc + c, i : i + 1] = v[k, row : row + 1]
                    if i in (0, X - 1):
                        sxy[slot, (2 if i else 0) + up, c : c + 1] = v[k, Y - 1 if up else 0][None]
        wide = 4 * unit
        go(made, (6, 7, 8, 9))
        for up in (0, 1):
            packed = jnp.zeros((8, Z), jnp.float32)
            for c in range(nc):
                at = wide * c * nx
                rolled = pltpu.roll(sy[slot, up, c], (at + 2 * unit) % Z, 1)
                packed = jnp.where(lane >= at, rolled, packed)
            syz[slot, up] = packed
        go(made, (10, 11, 12, 13))
        go(made, (2, 3))
        for t in range(T):
            packed = jnp.zeros((8, Z), jnp.float32)
            for c, v in enumerate(comps):
                for i in range(nx):
                    at = wide * (c * nx + i)
                    rolled = pltpu.roll(v[i, 8 * t : 8 * t + 8], (at + 2 * unit) % Z, 1)
                    packed = jnp.where(lane >= at, rolled, packed)
            sz[slot, t] = packed
        go(made, (14, 15, 16, 17, 0, 1, 4, 5))

    def rot(v, amount, axis):
        amount = amount % v.shape[axis]
        return pltpu.roll(v, amount, axis) if amount else v

    def near(below, above, unit):
        return jnp.where(lane % (4 * unit) < unit, rot(above, -2 * unit, 1), below)

    def unpack(tile, k, unit):
        return rot(tile, -unit - 4 * unit * k, 1)

    def stack(parts):
        return jnp.concatenate([q_[None] for q_ in parts], axis=0)

    def column(tiles, k, unit):
        return jnp.concatenate([unpack(tile, k, unit) for tile in tiles], axis=0)

    def six(v, hxm, hxp, hym, hyp, hz, unit):
        return (
            jnp.concatenate([v[1:], hxp[None]], axis=0),
            jnp.concatenate([hxm[None], v[:-1]], axis=0),
            jnp.where(iy >= Y - unit, hyp, pltpu.roll(v, Y - unit, 1)),
            jnp.where(iy < unit, hym, pltpu.roll(v, unit, 1)),
            jnp.where(iz >= Z - unit, hz, pltpu.roll(v, Z - unit, 2)),
            jnp.where(iz < unit, hz, pltpu.roll(v, unit, 2)),
        )

    def slab_rows(slab, nx):
        return [slab[i * X // nx : i * X // nx + 1] for i in range(nx)]

    def expand(flat, c):
        odd_z = iz[0] % 2 == 1
        odd_y = iy[0] % 2 == 1
        v = jnp.where(odd_z, flat, rot(flat, -1, 1)) if c == 2 else jnp.where(odd_z, rot(flat, 1, 1), flat)
        return jnp.where(odd_y, v, rot(v, -1, 0)) if c == 1 else jnp.where(odd_y, rot(v, 1, 0), v)

    def partial(v, coefs, extra, mass, unit):
        nx = v.shape[0]
        inn = extra[0]
        out = v * mass if mass != 1.0 else v
        out = out + inn[0] * (v - pltpu.roll(v, Y - unit, 1))
        out = out + inn[1] * (v - pltpu.roll(v, unit, 1))
        out = out + inn[2] * (v - pltpu.roll(v, Z - unit, 2))
        out = out + inn[3] * (v - pltpu.roll(v, unit, 2))
        flow = coefs[0][0, 1:nx] * (v[:-1] - v[1:])
        none = jnp.zeros((1, Y, Z), jnp.float32)
        return out + jnp.concatenate([flow, none], axis=0) - jnp.concatenate([none, flow], axis=0)

    def finish(ext, far_below, far_above, hy, hz, part, coefs, extra, mass, unit):
        nx = ext.shape[0] - 2
        v = ext[1 : nx + 1]
        cE, rim = coefs[0], extra[1]
        out = part + rim[1] * (v - hz[1 : nx + 1])
        out = out + rim[0] * (v - jnp.where(iy < Y // 2, hy[0][1 : nx + 1], hy[1][1 : nx + 1]))
        first = out[0:1] + cE[1, 1:2] * (v[0:1] - ext[0:1])
        final = out[nx - 1 :] + cE[0, nx : nx + 1] * (v[nx - 1 :] - ext[nx + 1 :])

        def sheet(k, beyond, before):
            e, h = ext[k : k + 1], hz[k : k + 1]
            nb = (
                beyond, before,
                jnp.where(iy >= Y - unit, hy[1][k : k + 1], pltpu.roll(e, Y - unit, 1)),
                jnp.where(iy < unit, hy[0][k : k + 1], pltpu.roll(e, unit, 1)),
                jnp.where(iz >= Z - unit, h, pltpu.roll(e, Z - unit, 2)),
                jnp.where(iz < unit, h, pltpu.roll(e, unit, 2)),
            )
            return stencil(e, nb, [cE[d, k : k + 1] for d in range(6)], mass)

        low = sheet(0, v[0:1], far_below[None])
        high = sheet(nx + 1, far_above[None], v[nx - 1 :])
        return jnp.concatenate([low, first, out[1 : nx - 1], final, high], axis=0)

    def land(slot, comps, unit, parts=None, work=None):
        nc, nx = len(comps), comps[0].shape[0]
        for n, ok, _, arrive in copies(slot, nc, nx):
            pl.when(ok)(arrive.wait_recv)
        wide = 4 * unit

        def xplane(c, up, layer):
            if nx == X:
                return rx[slot, up, layer * nc + c]
            flat = rx[slot, up, layer]
            if nc == 1:
                return flat
            return expand(flat, c)

        H1 = [near(rz[slot, 0, t], rz[slot, 1, t], unit) for t in range(T)]
        H2 = [jnp.where(lane % wide < unit, rot(rz[slot, 1, t], -3 * unit, 1), rot(rz[slot, 0, t], unit, 1))
              for t in range(T)]
        EX = [[near(rxz[slot, 2 * a, t], rxz[slot, 2 * a + 1, t], unit) for t in range(T)] for a in (0, 1)]
        EY = [near(ryz[slot, 2 * b], ryz[slot, 2 * b + 1], unit) for b in (0, 1)]
        field = {"E": [], "Y": [], "Z": H1}
        nbs = {"E": [], "Y": [], "Z": []}
        ux = X // nx
        for c, v in enumerate(comps):
            ext = jnp.concatenate([xplane(c, 0, 0)[None], v, xplane(c, 1, 0)[None]], axis=0)
            hy = []
            for b in (0, 1):
                hy.append(stack([rxy[slot, b, c : c + 1]] + slab_rows(ry[slot, b, c], nx) + [rxy[slot, 2 + b, c : c + 1]]))
            hz = stack([column(EX[0], c * nx + nx - 1, unit)] + [column(H1, c * nx + i, unit) for i in range(nx)]
                       + [column(EX[1], c * nx, unit)])
            field["E"].append(ext)
            if parts is None:
                nbs["E"].append(six(ext, xplane(c, 0, 1), xplane(c, 1, 1), hy[0], hy[1], hz, unit))
            else:
                nbs["E"].append(finish(ext, xplane(c, 0, 1), xplane(c, 1, 1), hy, hz, parts[c], *work, unit))
            fy, ny = [], []
            for b in (0, 1):
                slab = ry[slot, b, c]
                out, inner = ry[slot, b, nc + c], sy[slot, b, c]
                hzs = unpack(EY[b], c * nx, unit)
                fy.append(slab)
                ny.append((
                    jnp.where(sub >= 8 - ux, rxy[slot, 2 + b, c : c + 1], rot(slab, -ux, 0)),
                    jnp.where(sub < ux, rxy[slot, b, c : c + 1], rot(slab, ux, 0)),
                    out, inner,
                    jnp.where(lane >= Z - unit, hzs, rot(slab, -unit, 1)),
                    jnp.where(lane < unit, hzs, rot(slab, unit, 1)),
                ))
            field["Y"].append(fy)
            nbs["Y"].append(ny)
        which = lane // wide % nx
        rim = []
        for b in (0, 1):
            line = jnp.zeros((1, Z), jnp.float32)
            for i in range(nx):
                row = EY[b][i * ux : i * ux + 1]
                line = jnp.where(which[0:1] == i, rot(row, wide * i, 1), line)
            rim.append(line)
        for t in range(T):
            h = H1[t]
            before = rim[0] if t == 0 else rot(H1[t - 1], unit, 0)
            after = rim[1] if t == T - 1 else rot(H1[t + 1], -unit, 0)
            nbs["Z"].append((
                jnp.where(which == nx - 1, rot(EX[1][t], wide * (nx - 1), 1), rot(h, -wide, 1)),
                jnp.where(which == 0, rot(EX[0][t], -wide * (nx - 1), 1), rot(h, wide, 1)),
                jnp.where(sub >= 8 - unit, after, rot(h, -unit, 0)),
                jnp.where(sub < unit, before, rot(h, unit, 0)),
                H2[t],
                rot(sz[slot, t], -unit, 1),
            ))
        return field, nbs

    def stencil(v, nb, coef, mass):
        out = v * mass if mass != 1.0 else v
        for d in range(6):
            out = out + coef[d] * (v - nb[d])
        return out

    def viscous_wide(field, nbs, coefs, mass):
        cE, cY, cZ = coefs
        return {
            "E": nbs["E"],
            "Y": [[stencil(f[b], n[b], cY[b], mass) for b in (0, 1)] for f, n in zip(field["Y"], nbs["Y"])],
            "Z": [stencil(field["Z"][t], nbs["Z"][t], [cZ[d, t] for d in range(6)], mass) for t in range(T)],
        }

    def viscous(field, coefs, mass, unit):
        out = []
        for c in C:
            ext = field["E"][c]
            nx = ext.shape[0] - 2
            hy = [stack(slab_rows(field["Y"][c][b], nx)) for b in (0, 1)]
            hz = stack([column(field["Z"], c * nx + i, unit) for i in range(nx)])
            v = ext[1 : nx + 1]
            nb = six(v, ext[0], ext[nx + 1], hy[0], hy[1], hz, unit)
            out.append(stencil(v, nb, [coefs[0][d, 1 : nx + 1] for d in range(6)], mass))
        return out

    def fmap(fn, *fields):
        return {
            "E": [fn(*parts) for parts in zip(*(f["E"] for f in fields))],
            "Y": [[fn(*(f["Y"][c][b] for f in fields)) for b in (0, 1)] for c in range(len(fields[0]["Y"]))],
            "Z": [fn(*parts) for parts in zip(*(f["Z"] for f in fields))],
        }

    def flat_row(scalar, like):
        return scalar if like.ndim == 3 else scalar[0]

    def weights(E, Yw, Zw):
        return {"E": [E[...]] * NC, "Y": [[Yw[b] for b in (0, 1)]] * NC, "Z": [Zw[t] for t in range(T)]}

    def core(field):
        return [e[1 : e.shape[0] - 1] for e in field["E"]]

    def pairsum(v):
        v = v.reshape(X // 2, 2, Y, Z)
        v = v[:, 0] + v[:, 1]
        v = v + jnp.where(iy % 2 == 0, pltpu.roll(v, Y - 1, 1), pltpu.roll(v, 1, 1))
        return v + jnp.where(iz % 2 == 0, pltpu.roll(v, Z - 1, 2), pltpu.roll(v, 1, 2))

    def prolong(field):
        def deep(e):
            n = e.shape[0] - 2
            return jnp.concatenate([e[0:1]] + [e[1 + i : 2 + i] for i in range(n) for _ in (0, 1)] + [e[n + 1 :]], axis=0)

        def thin(h):
            m = lane % 8
            return jnp.where(m == 0, h, jnp.where(m == 1, rot(h, -1, 1), jnp.where(m == 4, rot(h, 4, 1), rot(h, 3, 1))))

        return {"E": [deep(e) for e in field["E"]], "Y": field["Y"], "Z": [thin(h) for h in field["Z"]]}

    inside = [jnp.where(exists(f), 1.0, 0.0).astype(jnp.float32) for f in faces]

    def set_up(field, nbs, nx, unit, mass, scale, E, Yc, Zc, wE, wY, wZ, extra):
        v = field["E"][0]
        ix = lax.broadcasted_iota(jnp.int32, v.shape, 0)
        keep = jnp.where(ix == 0, inside[0], jnp.where(ix == nx + 1, inside[1], 1.0))
        diag = jnp.full(v.shape, mass, jnp.float32)
        for d in range(6):
            face = scale * (v + nbs["E"][0][d]) * keep
            E[d] = face
            diag = diag + face
        wE[...] = relax / diag
        inn, rim = extra
        c2, c3, c4, c5 = (E[d, 1 : nx + 1] for d in range(2, 6))
        inn[0] = jnp.where(iy >= Y - unit, 0.0, c2)
        inn[1] = jnp.where(iy < unit, 0.0, c3)
        inn[2] = jnp.where(iz >= Z - unit, 0.0, c4)
        inn[3] = jnp.where(iz < unit, 0.0, c5)
        rim[0] = jnp.where(iy >= Y - unit, c2, jnp.where(iy < unit, c3, 0.0))
        rim[1] = jnp.where(iz >= Z - unit, c4, jnp.where(iz < unit, c5, 0.0))
        for b in (0, 1):
            v = field["Y"][0][b]
            diag = jnp.full(v.shape, mass, jnp.float32)
            for d in range(6):
                face = scale * (v + nbs["Y"][0][b][d]) * inside[2 + b]
                Yc[b, d] = face
                diag = diag + face
            wY[b] = relax / diag
        keep = jnp.where(lane % (4 * unit) < unit, inside[5], inside[4])
        span = 4 * unit * nx
        for t in range(T):
            v = field["Z"][t]
            diag = jnp.full(v.shape, mass, jnp.float32)
            for d in range(6):
                face = scale * (v + nbs["Z"][t][d]) * keep
                each = face
                for c in range(1, NC):
                    each = jnp.where(lane >= c * span, rot(face, c * span, 1), each)
                Zc[d, t] = each
                diag = diag + each
            wZ[t] = relax / diag

    fine = (cfE, cfY, cfZ)
    coarse = (ccE, ccY, ccZ)
    visc = v_ref[...]
    cvisc = pairsum(visc) * 0.125
    force = [f_ref[c] for c in C]
    pl.semaphore_wait(barrier, count)
    launch(0, [visc], 1)
    launch(1, force, 1)
    launch(2, [cvisc], 2)
    field, nbs = land(0, [visc], 1)
    set_up(field, nbs, X, 1, 1.0, 0.5, cfE, cfY, cfZ, fwE, fwY, fwZ, (fin, frim))
    field, nbs = land(2, [cvisc], 2)
    set_up(field, nbs, X // 2, 2, 8.0, 2.0, ccE, ccY, ccZ, cwE, cwY, cwZ, (cin, crim))
    forced, _ = land(1, force, 1)
    next_slot = [3]

    def take():
        next_slot[0] += 1
        return next_slot[0] - 1

    def pair(vec, middle):
        fw = weights(fwE, fwY, fwZ)
        cw = weights(cwE, cwY, cwZ)
        nxc = X // 2
        sm = fmap(lambda a, b: a * b, vec, fw)
        applied = viscous(sm, fine, 1.0, 1)
        cwl = cwE[1 : nxc + 1]
        local = core(vec)
        first = [cwl * pairsum(local[c] - applied[c]) for c in C]
        slot = take()
        launch(slot, first, 2)
        parts = [partial(v, *(coarse, (cin, crim), 8.0), 2) for v in first]
        one, nbs = land(slot, first, 2, parts, (coarse, (cin, crim), 8.0))
        two = fmap(lambda a, b, k: a + a - k * b, one, viscous_wide(one, nbs, coarse, 8.0), cw)
        applied = viscous(two, coarse, 8.0, 2)
        three = [v + first[c] - cwl * applied[c] for c, v in enumerate(core(two))]
        slot = take()
        launch(slot, three, 2)
        parts = [partial(v, *(coarse, (cin, crim), 8.0), 2) for v in three]
        middle()
        field, nbs = land(slot, three, 2, parts, (coarse, (cin, crim), 8.0))
        four = fmap(lambda a, o, b, k: a + o - k * b, field, one, viscous_wide(field, nbs, coarse, 8.0), cw)
        sm = fmap(lambda a, b: a + b, sm, prolong(four))
        applied = viscous(sm, fine, 1.0, 1)
        fwl = fwE[1 : X + 1]
        m = [v + fwl * (local[c] - applied[c]) for c, v in enumerate(core(sm))]
        slot = take()
        launch(slot, m, 1)
        parts = [partial(v, *(fine, (fin, frim), 1.0), 1) for v in m]
        field, nbs = land(slot, m, 1, parts, (fine, (fin, frim), 1.0))
        return m, viscous_wide(field, nbs, fine, 1.0)

    def red_copy(n, stage, k):
        if stage == 0:
            i, j = plane[k]
            peer, base = plane_peer(i, j), k
        else:
            peer, base = line_peer(k + 1), len(plane) + k
        return pltpu.make_async_remote_copy(
            src_ref=red_src.at[n, stage], dst_ref=red_dst.at[n, base],
            send_sem=rsend.at[n, base], recv_sem=rrecv.at[n, base],
            device_id=peer, device_id_type=MESH)

    def peers(stage):
        return range(len(plane)) if stage == 0 else range(gy_n - 1)

    def fold(v):
        v = v.reshape(X * T, 8, Z).sum(axis=0)
        return v + pltpu.roll(v, 4, 0)

    def reduce_start(n, r, u, w):
        g = d = 0.0
        for c in C:
            g = g + r[c] * u[c]
            d = d + u[c] * w[c]
        red_src[n, 0] = jnp.where(sub < 4, fold(g), fold(d))
        for k in peers(0):
            red_copy(n, 0, k).start()

    def reduce_middle(n):
        acc = red_src[n, 0]
        for k in peers(0):
            red_copy(n, 0, k).wait_recv()
            acc = acc + red_dst[n, k]
        red_src[n, 1] = acc
        for k in peers(1):
            red_copy(n, 1, k).start()

    def reduce_end(n):
        acc = red_src[n, 1]
        for k in peers(1):
            red_copy(n, 1, k).wait_recv()
            acc = acc + red_dst[n, len(plane) + k]
        g = jnp.sum(jnp.where(sub < 4, acc, 0.0))
        d = jnp.sum(jnp.where(sub < 4, 0.0, acc))
        return jnp.full((1, 1, Z), g), jnp.full((1, 1, Z), d)

    u, w = pair(forced, lambda: None)
    r = force
    gamma_old = alpha_old = None
    for n in range(ITERS):
        last = n == ITERS - 1
        wl = core(w)
        reduce_start(n, r, u, wl)
        if last:
            reduce_middle(n)
        else:
            m, nn = pair(w, lambda: reduce_middle(n))
        gamma, delta = reduce_end(n)
        if n == 0:
            alpha = gamma / delta
            p, s = u, wl
        else:
            beta = gamma / gamma_old
            alpha = gamma / (delta - beta * gamma / alpha_old)
            p = [u[c] + beta * p[c] for c in C]
            s = [wl[c] + beta * s[c] for c in C]
        for c in C:
            x_out[c] = alpha * p[c] if n == 0 else x_out[c] + alpha * p[c]
        r = [r[c] - alpha * s[c] for c in C]
        if last:
            for c in C:
                r_out[c] = r[c]
            break
        if n == 0:
            q, z = m, nn
        else:
            q = [m[c] + beta * q[c] for c in C]
            z = fmap(lambda a, b: a + flat_row(beta, a) * b, nn, z)
        u = [u[c] - alpha * q[c] for c in C]
        w = fmap(lambda a, b: a - flat_row(alpha, a) * b, w, z)
        gamma_old, alpha_old = gamma, alpha

    for slot, nc, nx in used:
        for _, ok, copy, _ in copies(slot, nc, nx):
            pl.when(ok)(copy.wait_send)
    for n in range(ITERS):
        for stage in (0, 1):
            for k in peers(stage):
                red_copy(n, stage, k).wait_send()


def solution(mesh):
    sizes = dict(mesh.shape)

    def shards(forcing, viscosity):
        NC, X, Y, Z = forcing.shape
        T = Y // 8
        f32 = jnp.float32
        peers = sizes["gx"] * sizes["gz"] - 1 + sizes["gy"] - 1
        spec = pl.BlockSpec(memory_space=pltpu.VMEM)
        out = jax.ShapeDtypeStruct(forcing.shape, f32)
        dma = pltpu.SemaphoreType.DMA
        V = lambda *shape: pltpu.VMEM(shape, f32)
        coefs = lambda nx: [V(6, nx + 2, Y, Z), V(2, 6, 8, Z), V(6, T, 8, Z)]
        weights = lambda nx: [V(nx + 2, Y, Z), V(2, 8, Z), V(T, 8, Z)]
        halo = [V(ROUNDS, 2, 2 * NC, Y, Z), V(ROUNDS, 2, 2 * NC, 8, Z)]
        return pl.pallas_call(
            functools.partial(kernel, sizes),
            out_shape=(out, out),
            in_specs=[spec, spec],
            out_specs=(spec, spec),
            scratch_shapes=halo + [V(ROUNDS, T, 8, Z), V(ROUNDS, 4, 8, Z), V(ROUNDS, 2, 8, Z)]
            + halo + [V(ROUNDS, 2, T, 8, Z), V(ROUNDS, 4, 8, Z), V(ROUNDS, 4, 8, Z), V(ROUNDS, 4, T, 8, Z)]
            + coefs(X) + weights(X) + coefs(X // 2) + weights(X // 2)
            + [V(4, X, Y, Z), V(2, X, Y, Z), V(4, X // 2, Y, Z), V(2, X // 2, Y, Z)] + [
                dma((ROUNDS, 18)),
                dma((ROUNDS, 18)),
                V(ITERS, 2, 8, Z),
                V(ITERS, peers, 8, Z),
                dma((ITERS, peers)),
                dma((ITERS, peers)),
            ],
            compiler_params=pltpu.CompilerParams(
                collective_id=0, has_side_effects=True, vmem_limit_bytes=48 * 1024 * 1024
            ),
        )(forcing, viscosity)

    return jax.shard_map(
        shards,
        mesh=mesh,
        in_specs=(P(None, "gx", "gy", "gz"), P("gx", "gy", "gz")),
        out_specs=(P(None, "gx", "gy", "gz"), P(None, "gx", "gy", "gz")),
        check_vma=False,
    )
```
